32 devices in a mesh: dp: 8 (over z, x), tensor: 4 (over y, core).
Axes of the slice: x: 2, y: 2, z: 4, core: 2. Of those that a mesh axis runs over, the one named last changes fastest.
Arguments:
- hidden_in: bfloat16 [32, 128, 4096], P(('dp', 'tensor')), parts along dimension 0, may hold values from -6 to 6
- norm_gain: float32 [4096], replicated, may hold values from 0.1 to 1.9
- query_weight: bfloat16 [4096, 4096], P(None, 'tensor'), may hold values from -3 to 3
- kv_weight: bfloat16 [4096, 2048], P(None, 'tensor'), may hold values from -3 to 3
- output_weight: bfloat16 [4096, 4096], P('tensor'), may hold values from -0.09375 to 0.09375
Outputs:
- attention_out: bfloat16 [32, 128, 4096], P(('dp', 'tensor')), parts along dimension 0
The draws below stay inside these ranges and needn't reach their ends.
There are 8 independent parts, one for each index of `dp`. The reference program is written for one: setup_inputs(seed, part) draws one part's arguments, and reference() takes and returns one part's arrays. A program takes and returns all parts, laid end to end along the dimension named above; an argument that names none is the same for every part. Nothing has to cross between parts.
All inputs are finite; a program needn't handle non-finite values.
Results may differ from the reference program's by a relative error of at most 0.014.
The reference program's roundings to bfloat16 on the way (of `normed`, `probabilities` and `mixed`) count: a program that leaves them out, or rounds other values in their place, can miss the bound.
Values may be sent and summed in bfloat16 or wider, within the bound.
A program may use at most 128 MiB of HBM per device.

```python
import math
import jax
import jax.numpy as jnp
from jax import lax

D = 4096
H = 32
KVH = 8
HD = 128
SEQ_LEN = 128
SEQS = 4


def projection_base(key):
    base = jnp.clip(jax.random.normal(jax.random.fold_in(key, 11), (D, H * HD), jnp.float32), -4.0, 4.0)
    return base


def draw_query_weight(key, part):
    base = projection_base(key)
    return (base * D ** (-0.5)).astype(jnp.bfloat16)


def draw_kv_weight(key, part):
    own_part = jnp.clip(jax.random.normal(jax.random.fold_in(key, 13), (D, KVH * HD), jnp.float32), -4.0, 4.0)
    value_part = jnp.clip(jax.random.normal(jax.random.fold_in(key, 14), (D, KVH * HD), jnp.float32), -4.0, 4.0)
    key_part = own_part
    joined = jnp.stack((key_part.reshape(D, KVH, HD), value_part.reshape(D, KVH, HD)), axis=2)
    return (joined.reshape(D, 2 * KVH * HD) * D ** (-0.5)).astype(jnp.bfloat16)


def block_levels(key, shape, cuts, smallest, largest):
    gain = 1.0
    for axis_at, blocks in cuts:
        heights = jax.random.uniform(jax.random.fold_in(jax.random.fold_in(key, 6), axis_at), (blocks,), jnp.float32, smallest / len(cuts), largest / len(cuts))
        gain = gain * jnp.repeat(jnp.exp(heights), shape[axis_at] // blocks).reshape((-1,) + (1,) * (len(shape) - 1 - axis_at))
    return gain


def noise(rng, dims, spread, most, shards=(), held_as=jnp.bfloat16):
    values = spread * jax.random.normal(rng, dims, jnp.float32)
    if shards:
        values = values * block_levels(rng, dims, shards, -0.22, 0.18)
    return jnp.clip(values, -most, most).astype(held_as)


def setup_inputs(seed: int = 0, part: int = 0) -> dict:
    seeds = jax.random.split(jax.random.key(seed), 6)
    own_keys = jax.random.split(jax.random.fold_in(seeds[5], part), 6)
    hidden_in = noise(own_keys[0], (SEQS, SEQ_LEN, D), 1.0, 6.0, ((0, 4),))
    norm_gain = jnp.clip(1.0 + 0.18 * jax.random.normal(seeds[1], (D,), jnp.float32), 0.1, 1.9)
    query_weight = draw_query_weight(jax.random.fold_in(seeds[5], 71), part)
    kv_weight = draw_kv_weight(jax.random.fold_in(seeds[5], 71), part)
    output_weight = noise(seeds[4], (H * HD, D), (H * HD) ** -0.5, 0.09375, ((0, 4),))
    return {"hidden_in": hidden_in, "norm_gain": norm_gain, "query_weight": query_weight, "kv_weight": kv_weight, "output_weight": output_weight}


EPS = 1e-05
THETA = 500000.0

def rotary(tensor, positions):
    half_width = tensor.shape[-1] // 2
    frequency = THETA ** (-(jnp.arange(half_width, dtype=jnp.float32) * 2.0 / tensor.shape[-1]))
    angles = positions[:, None] * frequency[None, :]
    cosine = jnp.cos(angles)[:, None, :]
    sine_part = jnp.sin(angles)[:, None, :]
    first_half = tensor[..., :half_width]
    second_half = tensor[..., half_width:]
    return jnp.concatenate((first_half * cosine - second_half * sine_part, second_half * cosine + first_half * sine_part), axis=-1)

def rms_norm(hidden_in, norm_gain):
    wide = hidden_in.astype(jnp.float32)
    mean_square = lax.optimization_barrier(jnp.mean(wide * wide, axis=-1, keepdims=True))
    return (wide * lax.rsqrt(mean_square + EPS) * norm_gain).astype(jnp.bfloat16)

def attend(queries, keys, values):
    length = queries.shape[1]
    scores = jnp.einsum('bqhgd,bkhd->bhgqk', queries.astype(jnp.float32), keys.astype(jnp.float32)) / math.sqrt(queries.shape[-1])
    causal = jnp.arange(length)[:, None] >= jnp.arange(length)[None, :]
    scores = jnp.where(causal, scores, -1e+30)
    highest = lax.optimization_barrier(jnp.max(scores, axis=-1, keepdims=True))
    exponent = jnp.exp(scores - highest)
    probabilities = (exponent / lax.optimization_barrier(jnp.sum(exponent, axis=-1, keepdims=True))).astype(jnp.bfloat16)
    mixed = jnp.einsum('bhgqk,bkhd->bqhgd', probabilities.astype(jnp.float32), values.astype(jnp.float32))
    return mixed.astype(jnp.bfloat16)

def reference(hidden_in, norm_gain, query_weight, kv_weight, output_weight):
    normed = rms_norm(hidden_in, norm_gain).astype(jnp.float32)
    queries_raw = jnp.einsum('bld,dc->blc', normed, query_weight.astype(jnp.float32))
    kv_raw = jnp.einsum('bld,dc->blc', normed, kv_weight.astype(jnp.float32)).astype(jnp.bfloat16)
    kv_split = kv_raw.reshape(SEQS, SEQ_LEN, KVH, 2, HD)
    keys_raw = kv_split[:, :, :, 0, :]
    values = kv_split[:, :, :, 1, :]
    positions = jnp.arange(SEQ_LEN, dtype=jnp.float32)
    queries = rotary(queries_raw.reshape(SEQS, SEQ_LEN, H, HD), positions).astype(jnp.bfloat16)
    keys_wide = lax.optimization_barrier(keys_raw).astype(jnp.float32)
    keys = rotary(keys_wide, positions).astype(jnp.bfloat16)
    mixed = attend(queries.reshape(SEQS, SEQ_LEN, KVH, H // KVH, HD), keys, values)
    result = jnp.einsum('blc,cd->bld', mixed.reshape(SEQS, SEQ_LEN, H * HD).astype(jnp.float32), output_weight.astype(jnp.float32))
    return result.astype(jnp.bfloat16)
```

```python
import functools
import math

import jax
import jax.numpy as jnp
from jax import lax
import numpy as np
from jax.experimental import pallas as pl
from jax.experimental.pallas import tpu as pltpu
from jax.sharding import PartitionSpec as P

KVH = 8
HD = 128


EPS = 1e-05
THETA = 500000.0


def partner_2(value, axis, bit):
    mask = 2**bit
    pairs = [(source, source ^ mask) for source in range(lax.axis_size(axis))]
    return lax.ppermute(value, axis, pairs)


def rotary(tensor, positions):
    half_width = tensor.shape[-1] // 2
    frequency = THETA ** (-(jnp.arange(half_width, dtype=jnp.float32) * 2.0 / tensor.shape[-1]))
    angles = positions[:, None] * frequency[None, :]
    cosine = jnp.cos(angles)[:, None, :]
    sine_part = jnp.sin(angles)[:, None, :]
    first_half = tensor[..., :half_width]
    second_half = tensor[..., half_width:]
    return jnp.concatenate(
        (
            first_half * cosine - second_half * sine_part,
            second_half * cosine + first_half * sine_part,
        ),
        axis=-1,
    )


def rms_norm(hidden_in, norm_gain):
    wide = hidden_in.astype(jnp.float32)
    mean_square = jnp.mean(wide * wide, axis=-1, keepdims=True)
    return (wide * lax.rsqrt(mean_square + EPS) * norm_gain).astype(jnp.bfloat16)


def attend(queries, keys, values):
    length = queries.shape[1]
    scores = jnp.einsum(
        "bqhgd,bkhd->bhgqk", queries, keys, preferred_element_type=jnp.float32
    ) / math.sqrt(queries.shape[-1])
    causal = jnp.arange(length)[:, None] >= jnp.arange(length)[None, :]
    scores = jnp.where(causal, scores, -1e30)
    highest = jnp.max(scores, axis=-1, keepdims=True)
    exponent = jnp.exp(scores - highest)
    probabilities = (exponent / jnp.sum(exponent, axis=-1, keepdims=True)).astype(jnp.bfloat16)
    mixed = jnp.einsum(
        "bhgqk,bkhd->bqhgd", probabilities, values, preferred_element_type=jnp.float32
    )
    return mixed.astype(jnp.bfloat16)


def join_heads(stacked, axis_dim):
    sharers = max(lax.axis_size("tensor") // KVH, 1)
    position = lax.axis_index("tensor")
    for bit_index in range(sharers.bit_length() - 1):
        partner = partner_2(stacked, "tensor", bit_index)
        keeps_first = position // (1 << bit_index) % 2 == 0
        stacked = jnp.where(
            keeps_first,
            jnp.concatenate((stacked, partner), axis_dim),
            jnp.concatenate((partner, stacked), axis_dim),
        )
    return stacked


def general_shards(hidden_in, norm_gain, query_weight, kv_weight, output_weight):
    merged_weight = jnp.concatenate((query_weight, kv_weight), axis=1)
    query_cols = query_weight.shape[1]
    normed = rms_norm(hidden_in, norm_gain)
    projected = jnp.einsum(
        "brd,dc->brc",
        lax.all_gather(normed, "tensor", axis=0, tiled=True),
        merged_weight,
        preferred_element_type=jnp.float32,
    )
    batch, length = (projected.shape[0], projected.shape[1])
    queries_raw = projected[..., :query_cols]
    kv_raw = projected[..., query_cols:].astype(jnp.bfloat16)
    kv_raw = join_heads(kv_raw, 2)
    kv_heads = kv_raw.shape[-1] // (2 * HD)
    kv_split = kv_raw.reshape(batch, length, kv_heads, 2, HD)
    keys_raw = kv_split[:, :, :, 0, :]
    values = kv_split[:, :, :, 1, :]
    heads = query_cols // HD
    positions = jnp.arange(length, dtype=jnp.float32)
    queries = rotary(queries_raw.reshape(batch, length, heads, HD), positions).astype(jnp.bfloat16)
    keys = rotary(keys_raw.astype(jnp.float32), positions).astype(jnp.bfloat16)
    mixed = attend(queries.reshape(batch, length, kv_heads, heads // kv_heads, HD), keys, values)
    mixed_rows = mixed.reshape(batch, length, heads * HD)
    partial_out = jnp.einsum(
        "blc,cd->bld", mixed_rows, output_weight, preferred_element_type=jnp.float32
    )
    return lax.psum_scatter(
        partial_out.astype(jnp.bfloat16), "tensor", scatter_dimension=0, tiled=True
    )


MESH = pl.DeviceIdType.MESH
CORES = 2
HALVES = 2
PIECES = 2
LAG = 3
OUT_TILES = 8
LAST_TILES = 1
FIRST_ROWS = 16


def rotary_tables(length):
    half = HD // 2
    frequency = np.float32(THETA) ** (-(np.arange(half, dtype=np.float32) * np.float32(2.0 / HD)))
    angles = np.arange(length, dtype=np.float32)[:, None] * frequency[None, :].astype(np.float32)
    cosine, sine = np.cos(angles), np.sin(angles)
    return np.stack(
        (np.concatenate((cosine, cosine), axis=1), np.concatenate((-sine, sine), axis=1))
    ).astype(np.float32)


def block_kernel(
    dims,
    hid, gain_in, wq_in, wkv_in, wo_in, table_in,
    out,
    gain, table,
    x, xn, wkv, wq, wo, qs, ks, vs, mixed_own, mixed_far,
    give, got, held, summed, landed, own_acc, own_give, own_got,
    small_sem, w_sem, sib_sem, far_send, far_recv, fwd_send, fwd_recv,
    give_send, give_recv, sum_send, sum_recv, own_sem,
):
    length, kvh, group, q_tiles, o_width = dims
    part = length // HALVES
    piece = part // PIECES
    me = lax.axis_index("tensor")
    sibling = me + 1 - 2 * lax.rem(me, CORES)
    across = lax.rem(me + CORES, 2 * CORES)

    def remote(src, dst, send, recv, target):
        return pltpu.make_async_remote_copy(
            src_ref=src, dst_ref=dst, send_sem=send, recv_sem=recv,
            device_id={"tensor": target}, device_id_type=MESH,
        )

    q_cols = q_tiles * HD
    kv_copy = pltpu.make_async_copy(wkv_in, wkv, w_sem.at[0])
    q_copies = [
        pltpu.make_async_copy(
            wq_in.at[:, pl.ds(i * q_cols, q_cols)], wq.at[:, pl.ds(i * q_cols, q_cols)], w_sem.at[1 + i]
        )
        for i in range(2)
    ]
    o_copy = pltpu.make_async_copy(wo_in, wo, w_sem.at[3])
    x_copy = pltpu.make_async_copy(hid.at[0], x.at[0], small_sem.at[0])
    gain_copy = pltpu.make_async_copy(gain_in, gain, small_sem.at[1])
    table_copy = pltpu.make_async_copy(table_in, table, small_sem.at[2])
    sib_copy = remote(x.at[0], x.at[1], sib_sem.at[0], sib_sem.at[1], sibling)

    def far_copy(src, row0, rows, p):
        at = pl.ds(row0, rows)
        return remote(src.at[0, at], x.at[2, at], far_send, far_recv.at[p], across)

    def fwd_copy(row0, rows, p):
        at = pl.ds(row0, rows)
        return remote(x.at[2, at], x.at[3, at], fwd_send, fwd_recv.at[p], sibling)

    def give_copy(h, j):
        return remote(give.at[h, j], got.at[h, j], give_send, give_recv.at[j], sibling)

    def sum_copy(h, j, count, i):
        at = pl.ds(j, count)
        return remote(summed.at[h, at], landed.at[h, at], sum_send, sum_recv.at[i], across)

    def own_copy(j, count):
        at = pl.ds(j, count)
        return remote(own_give.at[at], own_got.at[at], own_sem.at[0], own_sem.at[1], sibling)

    barrier = pltpu.get_barrier_semaphore()
    for target in (across, sibling):
        pl.semaphore_signal(barrier, inc=1, device_id={"tensor": target}, device_id_type=MESH)
    x_copy.start()
    gain_copy.start()
    table_copy.start()
    pl.semaphore_wait(barrier, 2)
    far_copy(hid, 0, FIRST_ROWS, 0).start()
    x_copy.wait()
    far_copy(x, FIRST_ROWS, piece - FIRST_ROWS, 0).start()
    for p in range(1, HALVES * PIECES):
        far_copy(x, p * piece, piece, p).start()
    sib_copy.start()
    kv_copy.start()
    for q_copy in q_copies:
        q_copy.start()
    o_copy.start()

    def normalise(slot, row0, rows, dst0):
        step = 16

        def body(i, carry):
            at = pl.multiple_of(i * step, step)
            wide = x[slot, pl.ds(row0 + at, step), :].astype(jnp.float32)
            mean_square = jnp.mean(wide * wide, axis=-1, keepdims=True)
            scaled = wide * lax.rsqrt(mean_square + EPS) * gain[...]
            xn[pl.ds(dst0 + at, step), :] = scaled.astype(jnp.bfloat16)
            return carry

        lax.fori_loop(0, rows // step, body, 0)

    def rotate(value, row0, rows):
        c = table[0, row0 : row0 + rows, :]
        s = table[1, row0 : row0 + rows, :]
        return value * c + pltpu.roll(value, HD // 2, 1) * s

    def columns(t, width):
        return pl.ds(pl.multiple_of(t * width, width), width)

    def project(slot0, row0, rows, first):
        both = 2 * rows

        def kv_body(g, carry):
            raw = jnp.dot(
                xn[:both, :], wkv[:, columns(g, 2 * HD)], preferred_element_type=jnp.float32
            ).astype(jnp.bfloat16)
            for s in range(2):
                mine = raw[s * rows : (s + 1) * rows]
                keys = rotate(mine[:, :HD].astype(jnp.float32), row0, rows)
                ks[slot0 + s, g, row0 : row0 + rows, :] = keys.astype(jnp.bfloat16)
                vs[slot0 + s, g, row0 : row0 + rows, :] = mine[:, HD:]
            return carry

        def q_body(t, carry):
            raw = jnp.dot(xn[:both, :], wq[:, columns(t, 2 * HD)], preferred_element_type=jnp.float32)
            for s in range(2):
                for e in range(2):
                    value = raw[s * rows : (s + 1) * rows, e * HD : (e + 1) * HD]
                    qs[s, 2 * t + e, :rows, :] = rotate(value, row0, rows).astype(jnp.bfloat16)
            return carry

        if first:
            kv_copy.wait()
        lax.fori_loop(0, kvh, kv_body, 0)
        if first:
            for i in range(2):
                q_copies[i].wait()
                lax.fori_loop(i * q_tiles // 2, (i + 1) * q_tiles // 2, q_body, 0)
        else:
            lax.fori_loop(0, q_tiles, q_body, 0)

    def attention(slot0, row0, rows, mixed):
        seen = row0 + rows
        for s in range(2):
            for g in range(kvh):
                queries = qs[s, g * group : (g + 1) * group, :rows, :].reshape(group * rows, HD)
                keys = ks[slot0 + s, g, :seen, :]
                scores = lax.dot_general(
                    queries, keys, (((1,), (1,)), ((), ())), preferred_element_type=jnp.float32
                ) * (1.0 / math.sqrt(HD))
                scores = scores.reshape(group, rows, seen)
                position = row0 + lax.broadcasted_iota(jnp.int32, (group, rows, seen), 1)
                key_at = lax.broadcasted_iota(jnp.int32, (group, rows, seen), 2)
                scores = jnp.where(position >= key_at, scores, -1e30)
                highest = jnp.max(scores, axis=-1, keepdims=True)
                exponent = jnp.exp(scores - highest)
                total = jnp.sum(exponent, axis=-1, keepdims=True)
                probabilities = (exponent * (1.0 / total)).astype(jnp.bfloat16)
                result = jnp.dot(
                    probabilities.reshape(group * rows, seen),
                    vs[slot0 + s, g, :seen, :],
                    preferred_element_type=jnp.float32,
                ).astype(jnp.bfloat16)
                for e in range(group):
                    head = g * group + e
                    mixed[s * rows : (s + 1) * rows, head * HD : (head + 1) * HD] = result[
                        e * rows : (e + 1) * rows
                    ]

    gain_copy.wait()
    table_copy.wait()
    normalise(0, 0, length, 0)
    sib_copy.wait_recv()
    normalise(1, 0, length, length)
    project(0, 0, length, True)
    attention(0, 0, length, mixed_own)

    def own_out(j, carry):
        partial = jnp.dot(
            mixed_own[...], wo[:, columns(j, o_width)], preferred_element_type=jnp.float32
        )
        own_acc[j] = partial[:length]
        own_give[j] = partial[length:].astype(jnp.bfloat16)
        own_copy(j, 1).start()
        return carry

    o_copy.wait()
    lax.fori_loop(0, OUT_TILES, own_out, 0)

    for h in range(HALVES):
        row0 = h * part
        for p in range(PIECES):
            at = p * piece
            far_copy(x, row0 + at, piece, h * PIECES + p).wait_recv()
            fwd_copy(row0 + at, piece, h * PIECES + p).start()
            normalise(2, row0 + at, piece, at)
        for p in range(PIECES):
            at = p * piece
            fwd_copy(row0 + at, piece, h * PIECES + p).wait_recv()
            normalise(3, row0 + at, piece, part + at)
        project(2, row0, part, False)
        attention(2, row0, part, mixed_far)

        def far_out(j, carry, h=h):
            @pl.when(j < OUT_TILES)
            def _():
                partial = jnp.dot(
                    mixed_far[...], wo[:, columns(j, o_width)], preferred_element_type=jnp.float32
                )
                held[j] = partial[:part]
                give[h, j] = partial[part:].astype(jnp.bfloat16)
                give_copy(h, j).start()

            @pl.when(j >= LAG)
            def _():
                t = j - LAG
                give_copy(h, t).wait_recv()
                summed[h, t] = (held[t] + got[h, t].astype(jnp.float32)).astype(jnp.bfloat16)
                if h < HALVES - 1:
                    sum_copy(h, t, 1, h).start()
                else:
                    late = (t >= OUT_TILES - LAST_TILES).astype(jnp.int32)
                    sum_copy(h, t, 1, h + late).start()

            return carry

        lax.fori_loop(0, OUT_TILES + LAG, far_out, 0)

    own_copy(0, OUT_TILES).wait_recv()

    def join(j, carry):
        own_acc[j] = own_acc[j] + own_got[j].astype(jnp.float32)
        return carry

    lax.fori_loop(0, OUT_TILES, join, 0)

    spans = [(h, 0, OUT_TILES) for h in range(HALVES - 1)]
    spans += [(HALVES - 1, 0, OUT_TILES - LAST_TILES), (HALVES - 1, OUT_TILES - LAST_TILES, LAST_TILES)]
    for i, (h, j0, count) in enumerate(spans):

        def finish(j, carry, h=h):
            rows = pl.ds(h * part, part)
            out[0, rows, columns(j, o_width)] = (
                own_acc[j, rows, :] + landed[h, j].astype(jnp.float32)
            ).astype(jnp.bfloat16)
            return carry

        sum_copy(h, j0, count, i).wait_recv()
        lax.fori_loop(j0, j0 + count, finish, 0)

    own_copy(0, OUT_TILES).wait_send()
    remote(give, got, give_send, give_recv.at[0], sibling).wait_send()
    remote(summed, landed, sum_send, sum_recv.at[0], across).wait_send()
    sib_copy.wait_send()
    far_copy(x, 0, length, 0).wait_send()
    fwd_copy(0, length, 0).wait_send()


def paired_shards(hidden_in, norm_gain, query_weight, kv_weight, output_weight):
    _, length, width = hidden_in.shape
    query_cols, kv_cols = query_weight.shape[1], kv_weight.shape[1]
    heads, kvh = query_cols // HD, kv_cols // (2 * HD)
    q_tiles = query_cols // (2 * HD)
    part = length // HALVES
    o_width = width // OUT_TILES
    bf16, f32 = jnp.bfloat16, jnp.float32
    dma = pltpu.SemaphoreType.DMA
    any_spec = pl.BlockSpec(memory_space=pl.ANY)
    dims = (length, kvh, heads // kvh, q_tiles, o_width)
    return pl.pallas_call(
        functools.partial(block_kernel, dims),
        out_shape=pltpu.VMEM(hidden_in.shape, bf16),
        in_specs=[any_spec] * 6,
        out_specs=pl.BlockSpec(memory_space=pltpu.VMEM),
        scratch_shapes=[
            pltpu.VMEM((1, width), f32),
            pltpu.VMEM((2, length, HD), f32),
            pltpu.VMEM((4, length, width), bf16),
            pltpu.VMEM((2 * length, width), bf16),
            pltpu.VMEM((width, kv_cols), bf16),
            pltpu.VMEM((width, query_cols), bf16),
            pltpu.VMEM((query_cols, width), bf16),
            pltpu.VMEM((2, heads, length, HD), bf16),
            pltpu.VMEM((4, kvh, length, HD), bf16),
            pltpu.VMEM((4, kvh, length, HD), bf16),
            pltpu.VMEM((2 * length, query_cols), bf16),
            pltpu.VMEM((2 * part, query_cols), bf16),
            pltpu.VMEM((HALVES, OUT_TILES, part, o_width), bf16),
            pltpu.VMEM((HALVES, OUT_TILES, part, o_width), bf16),
            pltpu.VMEM((OUT_TILES, part, o_width), f32),
            pltpu.VMEM((HALVES, OUT_TILES, part, o_width), bf16),
            pltpu.VMEM((HALVES, OUT_TILES, part, o_width), bf16),
            pltpu.VMEM((OUT_TILES, length, o_width), f32),
            pltpu.VMEM((OUT_TILES, length, o_width), bf16),
            pltpu.VMEM((OUT_TILES, length, o_width), bf16),
            dma((3,)),
            dma((4,)),
            dma((2,)),
            dma, dma((HALVES * PIECES,)),
            dma, dma((HALVES * PIECES,)),
            dma, dma((OUT_TILES,)),
            dma, dma((HALVES + 1,)),
            dma((2,)),
        ],
        compiler_params=pltpu.CompilerParams(
            collective_id=0, has_side_effects=True, vmem_limit_bytes=60 * 2**20
        ),
    )(
        hidden_in, norm_gain.reshape(1, width), query_weight, kv_weight, output_weight,
        jnp.asarray(rotary_tables(length)),
    )


def shards(hidden_in, norm_gain, query_weight, kv_weight, output_weight):
    two_chips = lax.axis_size("tensor") == 2 * CORES
    whole_heads = kv_weight.shape[1] % (2 * HD) == 0
    if two_chips and whole_heads and hidden_in.shape[0] == 1:
        return paired_shards(hidden_in, norm_gain, query_weight, kv_weight, output_weight)
    return general_shards(hidden_in, norm_gain, query_weight, kv_weight, output_weight)


def solution(mesh):
    placed = (
        P(("dp", "tensor"), None, None),
        P(),
        P(None, "tensor"),
        P(None, "tensor"),
        P("tensor", None),
    )
    return jax.shard_map(
        shards,
        mesh=mesh,
        in_specs=placed,
        out_specs=P(("dp", "tensor"), None, None),
        check_vma=False,
    )
```

```python
import functools
import math

import jax
import jax.numpy as jnp
from jax import lax
import numpy as np
from jax.experimental import pallas as pl
from jax.experimental.pallas import tpu as pltpu
from jax.sharding import PartitionSpec as P

KVH = 8
HD = 128


EPS = 1e-05
THETA = 500000.0


def partner_2(value, axis, bit):
    mask = 2**bit
    pairs = [(source, source ^ mask) for source in range(lax.axis_size(axis))]
    return lax.ppermute(value, axis, pairs)


def rotary(tensor, positions):
    half_width = tensor.shape[-1] // 2
    frequency = THETA ** (-(jnp.arange(half_width, dtype=jnp.float32) * 2.0 / tensor.shape[-1]))
    angles = positions[:, None] * frequency[None, :]
    cosine = jnp.cos(angles)[:, None, :]
    sine_part = jnp.sin(angles)[:, None, :]
    first_half = tensor[..., :half_width]
    second_half = tensor[..., half_width:]
    return jnp.concatenate(
        (
            first_half * cosine - second_half * sine_part,
            second_half * cosine + first_half * sine_part,
        ),
        axis=-1,
    )


def rms_norm(hidden_in, norm_gain):
    wide = hidden_in.astype(jnp.float32)
    mean_square = jnp.mean(wide * wide, axis=-1, keepdims=True)
    return (wide * lax.rsqrt(mean_square + EPS) * norm_gain).astype(jnp.bfloat16)


def attend(queries, keys, values):
    length = queries.shape[1]
    scores = jnp.einsum(
        "bqhgd,bkhd->bhgqk", queries, keys, preferred_element_type=jnp.float32
    ) / math.sqrt(queries.shape[-1])
    causal = jnp.arange(length)[:, None] >= jnp.arange(length)[None, :]
    scores = jnp.where(causal, scores, -1e30)
    highest = jnp.max(scores, axis=-1, keepdims=True)
    exponent = jnp.exp(scores - highest)
    probabilities = (exponent / jnp.sum(exponent, axis=-1, keepdims=True)).astype(jnp.bfloat16)
    mixed = jnp.einsum(
        "bhgqk,bkhd->bqhgd", probabilities, values, preferred_element_type=jnp.float32
    )
    return mixed.astype(jnp.bfloat16)


def join_heads(stacked, axis_dim):
    sharers = max(lax.axis_size("tensor") // KVH, 1)
    position = lax.axis_index("tensor")
    for bit_index in range(sharers.bit_length() - 1):
        partner = partner_2(stacked, "tensor", bit_index)
        keeps_first = position // (1 << bit_index) % 2 == 0
        stacked = jnp.where(
            keeps_first,
            jnp.concatenate((stacked, partner), axis_dim),
            jnp.concatenate((partner, stacked), axis_dim),
        )
    return stacked


def general_shards(hidden_in, norm_gain, query_weight, kv_weight, output_weight):
    merged_weight = jnp.concatenate((query_weight, kv_weight), axis=1)
    query_cols = query_weight.shape[1]
    normed = rms_norm(hidden_in, norm_gain)
    projected = jnp.einsum(
        "brd,dc->brc",
        lax.all_gather(normed, "tensor", axis=0, tiled=True),
        merged_weight,
        preferred_element_type=jnp.float32,
    )
    batch, length = (projected.shape[0], projected.shape[1])
    queries_raw = projected[..., :query_cols]
    kv_raw = projected[..., query_cols:].astype(jnp.bfloat16)
    kv_raw = join_heads(kv_raw, 2)
    kv_heads = kv_raw.shape[-1] // (2 * HD)
    kv_split = kv_raw.reshape(batch, length, kv_heads, 2, HD)
    keys_raw = kv_split[:, :, :, 0, :]
    values = kv_split[:, :, :, 1, :]
    heads = query_cols // HD
    positions = jnp.arange(length, dtype=jnp.float32)
    queries = rotary(queries_raw.reshape(batch, length, heads, HD), positions).astype(jnp.bfloat16)
    keys = rotary(keys_raw.astype(jnp.float32), positions).astype(jnp.bfloat16)
    mixed = attend(queries.reshape(batch, length, kv_heads, heads // kv_heads, HD), keys, values)
    mixed_rows = mixed.reshape(batch, length, heads * HD)
    partial_out = jnp.einsum(
        "blc,cd->bld", mixed_rows, output_weight, preferred_element_type=jnp.float32
    )
    return lax.psum_scatter(
        partial_out.astype(jnp.bfloat16), "tensor", scatter_dimension=0, tiled=True
    )


MESH = pl.DeviceIdType.MESH
CORES = 2
HALVES = 2
PIECES = 2
LAG = 3
OUT_TILES = 8
LAST_TILES = 1
FIRST_ROWS = 16
RELAYS = (1, 2, 3, 4)
RELAY_TILE = 0


def rotary_tables(length):
    half = HD // 2
    frequency = np.float32(THETA) ** (-(np.arange(half, dtype=np.float32) * np.float32(2.0 / HD)))
    angles = np.arange(length, dtype=np.float32)[:, None] * frequency[None, :].astype(np.float32)
    cosine, sine = np.cos(angles), np.sin(angles)
    return np.stack(
        (np.concatenate((cosine, cosine), axis=1), np.concatenate((-sine, sine), axis=1))
    ).astype(np.float32)


def block_kernel(
    dims,
    hid, gain_in, wq_in, wkv_in, wo_in, table_in,
    out,
    gain, table,
    x, xn, wkv, wq, wo, qs, ks, vs, mixed_own, mixed_far,
    give, got, held, summed, landed, own_acc, own_give, own_got,
    small_sem, w_sem, sib_sem, far_send, far_recv, fwd_send, fwd_recv,
    give_send, give_recv, sum_send, sum_recv, own_sem, relay, relay_sem, relay_ready,
):
    length, kvh, group, q_tiles, o_width = dims
    part = length // HALVES
    piece = part // PIECES
    me = lax.axis_index("tensor")
    sibling = me + 1 - 2 * lax.rem(me, CORES)
    across = lax.rem(me + CORES, 2 * CORES)
    group_at = lax.axis_index("dp")
    relays = [r for r in RELAYS if r < lax.axis_size("dp")]
    relay_rows = part // max(len(relays), 1)
    is_target = (group_at == 0) & (me == 0)
    is_source = (group_at == 0) & (me == CORES)
    forwards = [(group_at == r) & (me == 0) for r in relays]

    def remote(src, dst, send, recv, target):
        return pltpu.make_async_remote_copy(
            src_ref=src, dst_ref=dst, send_sem=send, recv_sem=recv,
            device_id={"tensor": target}, device_id_type=MESH,
        )

    q_cols = q_tiles * HD
    kv_copy = pltpu.make_async_copy(wkv_in, wkv, w_sem.at[0])
    q_copies = [
        pltpu.make_async_copy(
            wq_in.at[:, pl.ds(i * q_cols, q_cols)], wq.at[:, pl.ds(i * q_cols, q_cols)], w_sem.at[1 + i]
        )
        for i in range(2)
    ]
    o_copy = pltpu.make_async_copy(wo_in, wo, w_sem.at[3])
    x_copy = pltpu.make_async_copy(hid.at[0], x.at[0], small_sem.at[0])
    gain_copy = pltpu.make_async_copy(gain_in, gain, small_sem.at[1])
    table_copy = pltpu.make_async_copy(table_in, table, small_sem.at[2])
    sib_copy = remote(x.at[0], x.at[1], sib_sem.at[0], sib_sem.at[1], sibling)

    def far_copy(src, row0, rows, p):
        at = pl.ds(row0, rows)
        return remote(src.at[0, at], x.at[2, at], far_send, far_recv.at[p], across)

    def fwd_copy(row0, rows, p):
        at = pl.ds(row0, rows)
        return remote(x.at[2, at], x.at[3, at], fwd_send, fwd_recv.at[p], sibling)

    def give_copy(h, j):
        return remote(give.at[h, j], got.at[h, j], give_send, give_recv.at[j], sibling)

    def sum_copy(h, j, count, i):
        at = pl.ds(j, count)
        return remote(summed.at[h, at], landed.at[h, at], sum_send, sum_recv.at[i], across)

    def relay_copy(i):
        at = pl.ds(i * relay_rows, relay_rows)
        return pltpu.make_async_remote_copy(
            src_ref=summed.at[HALVES - 1, RELAY_TILE, at], dst_ref=relay, send_sem=sum_send,
            recv_sem=relay_sem.at[0], device_id={"dp": relays[i], "tensor": 0}, device_id_type=MESH,
        )

    def forward_copy(i):
        at = pl.ds(i * relay_rows, relay_rows)
        return pltpu.make_async_remote_copy(
            src_ref=relay, dst_ref=landed.at[HALVES - 1, RELAY_TILE, at], send_sem=relay_sem.at[1],
            recv_sem=sum_recv.at[HALVES - 1], device_id={"dp": 0, "tensor": 0}, device_id_type=MESH,
        )

    def own_copy(j, count):
        at = pl.ds(j, count)
        return remote(own_give.at[at], own_got.at[at], own_sem.at[0], own_sem.at[1], sibling)

    barrier = pltpu.get_barrier_semaphore()
    for target in (across, sibling):
        pl.semaphore_signal(barrier, inc=1, device_id={"tensor": target}, device_id_type=MESH)
    for r in relays:

        @pl.when(is_target | is_source)
        def _(r=r):
            pl.semaphore_signal(
                barrier, inc=1, device_id={"dp": r, "tensor": 0}, device_id_type=MESH
            )

    x_copy.start()
    gain_copy.start()
    table_copy.start()
    peers = 2 + sum(2 * forwarding.astype(jnp.int32) for forwarding in forwards)
    pl.semaphore_wait(barrier, peers)
    for forwarding in forwards:

        @pl.when(forwarding)
        def _():
            pl.semaphore_signal(
                relay_ready, inc=1, device_id={"dp": 0, "tensor": CORES}, device_id_type=MESH
            )

    far_copy(hid, 0, FIRST_ROWS, 0).start()
    x_copy.wait()
    far_copy(x, FIRST_ROWS, piece - FIRST_ROWS, 0).start()
    for p in range(1, HALVES * PIECES):
        far_copy(x, p * piece, piece, p).start()
    sib_copy.start()
    kv_copy.start()
    for q_copy in q_copies:
        q_copy.start()
    o_copy.start()

    def normalise(slot, row0, rows, dst0):
        step = 16

        def body(i, carry):
            at = pl.multiple_of(i * step, step)
            wide = x[slot, pl.ds(row0 + at, step), :].astype(jnp.float32)
            mean_square = jnp.mean(wide * wide, axis=-1, keepdims=True)
            scaled = wide * lax.rsqrt(mean_square + EPS) * gain[...]
            xn[pl.ds(dst0 + at, step), :] = scaled.astype(jnp.bfloat16)
            return carry

        lax.fori_loop(0, rows // step, body, 0)

    def rotate(value, row0, rows):
        c = table[0, row0 : row0 + rows, :]
        s = table[1, row0 : row0 + rows, :]
        return value * c + pltpu.roll(value, HD // 2, 1) * s

    def columns(t, width):
        return pl.ds(pl.multiple_of(t * width, width), width)

    def project(slot0, row0, rows, first):
        both = 2 * rows

        def kv_body(g, carry):
            raw = jnp.dot(
                xn[:both, :], wkv[:, columns(g, 2 * HD)], preferred_element_type=jnp.float32
            ).astype(jnp.bfloat16)
            for s in range(2):
                mine = raw[s * rows : (s + 1) * rows]
                keys = rotate(mine[:, :HD].astype(jnp.float32), row0, rows)
                ks[slot0 + s, g, row0 : row0 + rows, :] = keys.astype(jnp.bfloat16)
                vs[slot0 + s, g, row0 : row0 + rows, :] = mine[:, HD:]
            return carry

        def q_body(t, carry):
            raw = jnp.dot(xn[:both, :], wq[:, columns(t, 2 * HD)], preferred_element_type=jnp.float32)
            for s in range(2):
                for e in range(2):
                    value = raw[s * rows : (s + 1) * rows, e * HD : (e + 1) * HD]
                    qs[s, 2 * t + e, :rows, :] = rotate(value, row0, rows).astype(jnp.bfloat16)
            return carry

        if first:
            kv_copy.wait()
        lax.fori_loop(0, kvh, kv_body, 0)
        if first:
            for i in range(2):
                q_copies[i].wait()
                lax.fori_loop(i * q_tiles // 2, (i + 1) * q_tiles // 2, q_body, 0)
        else:
            lax.fori_loop(0, q_tiles, q_body, 0)

    def attention(slot0, row0, rows, mixed):
        seen = row0 + rows
        for s in range(2):
            for g in range(kvh):
                queries = qs[s, g * group : (g + 1) * group, :rows, :].reshape(group * rows, HD)
                keys = ks[slot0 + s, g, :seen, :]
                scores = lax.dot_general(
                    queries, keys, (((1,), (1,)), ((), ())), preferred_element_type=jnp.float32
                ) * (1.0 / math.sqrt(HD))
                scores = scores.reshape(group, rows, seen)
                position = row0 + lax.broadcasted_iota(jnp.int32, (group, rows, seen), 1)
                key_at = lax.broadcasted_iota(jnp.int32, (group, rows, seen), 2)
                scores = jnp.where(position >= key_at, scores, -1e30)
                highest = jnp.max(scores, axis=-1, keepdims=True)
                exponent = jnp.exp(scores - highest)
                total = jnp.sum(exponent, axis=-1, keepdims=True)
                probabilities = (exponent * (1.0 / total)).astype(jnp.bfloat16)
                result = jnp.dot(
                    probabilities.reshape(group * rows, seen),
                    vs[slot0 + s, g, :seen, :],
                    preferred_element_type=jnp.float32,
                ).astype(jnp.bfloat16)
                for e in range(group):
                    head = g * group + e
                    mixed[s * rows : (s + 1) * rows, head * HD : (head + 1) * HD] = result[
                        e * rows : (e + 1) * rows
                    ]

    gain_copy.wait()
    table_copy.wait()
    normalise(0, 0, length, 0)
    sib_copy.wait_recv()
    normalise(1, 0, length, length)
    project(0, 0, length, True)
    attention(0, 0, length, mixed_own)

    def own_out(j, carry):
        partial = jnp.dot(
            mixed_own[...], wo[:, columns(j, o_width)], preferred_element_type=jnp.float32
        )
        own_acc[j] = partial[:length]
        own_give[j] = partial[length:].astype(jnp.bfloat16)
        own_copy(j, 1).start()
        return carry

    o_copy.wait()
    lax.fori_loop(0, OUT_TILES, own_out, 0)

    for h in range(HALVES):
        row0 = h * part
        for p in range(PIECES):
            at = p * piece
            far_copy(x, row0 + at, piece, h * PIECES + p).wait_recv()
            fwd_copy(row0 + at, piece, h * PIECES + p).start()
            normalise(2, row0 + at, piece, at)
        for p in range(PIECES):
            at = p * piece
            fwd_copy(row0 + at, piece, h * PIECES + p).wait_recv()
            normalise(3, row0 + at, piece, part + at)
        project(2, row0, part, False)
        attention(2, row0, part, mixed_far)

        def far_out(j, carry, h=h):
            @pl.when(j < OUT_TILES)
            def _():
                partial = jnp.dot(
                    mixed_far[...], wo[:, columns(j, o_width)], preferred_element_type=jnp.float32
                )
                held[j] = partial[:part]
                give[h, j] = partial[part:].astype(jnp.bfloat16)
                give_copy(h, j).start()

            @pl.when(j >= LAG)
            def _():
                t = j - LAG
                give_copy(h, t).wait_recv()
                summed[h, t] = (held[t] + got[h, t].astype(jnp.float32)).astype(jnp.bfloat16)
                if h < HALVES - 1:
                    sum_copy(h, t, 1, h).start()
                else:
                    late = (t >= OUT_TILES - LAST_TILES).astype(jnp.int32)
                    relayed = is_source & (t == RELAY_TILE) & (len(relays) > 0)

                    @pl.when(relayed)
                    def _():
                        pl.semaphore_wait(relay_ready, len(relays))
                        for i in range(len(relays)):
                            relay_copy(i).start()

                    @pl.when(jnp.logical_not(relayed))
                    def _():
                        sum_copy(h, t, 1, h + late).start()

            return carry

        lax.fori_loop(0, OUT_TILES + LAG, far_out, 0)

    own_copy(0, OUT_TILES).wait_recv()

    def join(j, carry):
        own_acc[j] = own_acc[j] + own_got[j].astype(jnp.float32)
        return carry

    lax.fori_loop(0, OUT_TILES, join, 0)
    for i, forwarding in enumerate(forwards):

        @pl.when(forwarding)
        def _(i=i):
            relay_copy(i).wait_recv()
            forward_copy(i).start()


    spans = [(h, 0, OUT_TILES) for h in range(HALVES - 1)]
    spans += [(HALVES - 1, 0, OUT_TILES - LAST_TILES), (HALVES - 1, OUT_TILES - LAST_TILES, LAST_TILES)]
    for i, (h, j0, count) in enumerate(spans):

        def finish(j, carry, h=h):
            rows = pl.ds(h * part, part)
            out[0, rows, columns(j, o_width)] = (
                own_acc[j, rows, :] + landed[h, j].astype(jnp.float32)
            ).astype(jnp.bfloat16)
            return carry

        sum_copy(h, j0, count, i).wait_recv()
        lax.fori_loop(j0, j0 + count, finish, 0)

    for i, forwarding in enumerate(forwards):

        @pl.when(forwarding)
        def _(i=i):
            forward_copy(i).wait_send()

    own_copy(0, OUT_TILES).wait_send()
    remote(give, got, give_send, give_recv.at[0], sibling).wait_send()
    remote(summed, landed, sum_send, sum_recv.at[0], across).wait_send()
    sib_copy.wait_send()
    far_copy(x, 0, length, 0).wait_send()
    fwd_copy(0, length, 0).wait_send()


def paired_shards(hidden_in, norm_gain, query_weight, kv_weight, output_weight):
    _, length, width = hidden_in.shape
    query_cols, kv_cols = query_weight.shape[1], kv_weight.shape[1]
    heads, kvh = query_cols // HD, kv_cols // (2 * HD)
    q_tiles = query_cols // (2 * HD)
    part = length // HALVES
    o_width = width // OUT_TILES
    relays = len([r for r in RELAYS if r < lax.axis_size("dp")])
    bf16, f32 = jnp.bfloat16, jnp.float32
    dma = pltpu.SemaphoreType.DMA
    any_spec = pl.BlockSpec(memory_space=pl.ANY)
    dims = (length, kvh, heads // kvh, q_tiles, o_width)
    return pl.pallas_call(
        functools.partial(block_kernel, dims),
        out_shape=pltpu.VMEM(hidden_in.shape, bf16),
        in_specs=[any_spec] * 6,
        out_specs=pl.BlockSpec(memory_space=pltpu.VMEM),
        scratch_shapes=[
            pltpu.VMEM((1, width), f32),
            pltpu.VMEM((2, length, HD), f32),
            pltpu.VMEM((4, length, width), bf16),
            pltpu.VMEM((2 * length, width), bf16),
            pltpu.VMEM((width, kv_cols), bf16),
            pltpu.VMEM((width, query_cols), bf16),
            pltpu.VMEM((query_cols, width), bf16),
            pltpu.VMEM((2, heads, length, HD), bf16),
            pltpu.VMEM((4, kvh, length, HD), bf16),
            pltpu.VMEM((4, kvh, length, HD), bf16),
            pltpu.VMEM((2 * length, query_cols), bf16),
            pltpu.VMEM((2 * part, query_cols), bf16),
            pltpu.VMEM((HALVES, OUT_TILES, part, o_width), bf16),
            pltpu.VMEM((HALVES, OUT_TILES, part, o_width), bf16),
            pltpu.VMEM((OUT_TILES, part, o_width), f32),
            pltpu.VMEM((HALVES, OUT_TILES, part, o_width), bf16),
            pltpu.VMEM((HALVES, OUT_TILES, part, o_width), bf16),
            pltpu.VMEM((OUT_TILES, length, o_width), f32),
            pltpu.VMEM((OUT_TILES, length, o_width), bf16),
            pltpu.VMEM((OUT_TILES, length, o_width), bf16),
            dma((3,)),
            dma((4,)),
            dma((2,)),
            dma, dma((HALVES * PIECES,)),
            dma, dma((HALVES * PIECES,)),
            dma, dma((OUT_TILES,)),
            dma, dma((HALVES + 1,)),
            dma((2,)),
            pltpu.VMEM((part // max(relays, 1), o_width), bf16),
            dma((2,)),
            pltpu.SemaphoreType.REGULAR,
        ],
        compiler_params=pltpu.CompilerParams(
            collective_id=0, has_side_effects=True, vmem_limit_bytes=60 * 2**20
        ),
    )(
        hidden_in, norm_gain.reshape(1, width), query_weight, kv_weight, output_weight,
        jnp.asarray(rotary_tables(length)),
    )


def shards(hidden_in, norm_gain, query_weight, kv_weight, output_weight):
    two_chips = lax.axis_size("tensor") == 2 * CORES
    whole_heads = kv_weight.shape[1] % (2 * HD) == 0
    if two_chips and whole_heads and hidden_in.shape[0] == 1:
        return paired_shards(hidden_in, norm_gain, query_weight, kv_weight, output_weight)
    return general_shards(hidden_in, norm_gain, query_weight, kv_weight, output_weight)


def solution(mesh):
    placed = (
        P(("dp", "tensor"), None, None),
        P(),
        P(None, "tensor"),
        P(None, "tensor"),
        P("tensor", None),
    )
    return jax.shard_map(
        shards,
        mesh=mesh,
        in_specs=placed,
        out_specs=P(("dp", "tensor"), None, None),
        check_vma=False,
    )
```
